64 devices in a mesh: dp: 4 (over x, y), sp: 16 (over z, core).
Axes of the slice: x: 2, y: 2, z: 8, core: 2. Of those that a mesh axis runs over, the one named last changes fastest.
The devices are a block of a 4x4x8 slice.
Arguments:
- tokens: bfloat16 [384, 4096], P('dp'), parts along dimension 0
- w_query: bfloat16 [4096, 4096], replicated
- w_key: bfloat16 [4096, 256], replicated
- w_value: bfloat16 [4096, 256], replicated
- w_out: bfloat16 [4096, 4096], P('sp')
- k_cache: bfloat16 [384, 1024, 256], P('dp', 'sp'), parts along dimension 0
- v_cache: bfloat16 [384, 1024, 256], P('dp', 'sp'), parts along dimension 0
- positions: int32 [384], P('dp'), parts along dimension 0
Outputs:
- output 1: bfloat16 [384, 4096], P('dp'), parts along dimension 0
- output 2: bfloat16 [384, 1024, 256], P('dp', 'sp'), parts along dimension 0
- output 3: bfloat16 [384, 1024, 256], P('dp', 'sp'), parts along dimension 0
There are 4 independent parts. The reference program is written for one: setup_inputs(seed, part) draws one part's arguments, and reference() takes and returns one part's arrays. A program takes and returns all parts, laid end to end along the dimension named above; an argument that names none is the same for every part.
All inputs are finite; a program needn't handle non-finite values.
Results may differ from the reference program's by a relative error of at most 0.00458535.
Values are sent between devices in bfloat16 or wider.
A program may use at most 768 MiB of HBM per device.

```python
import jax
import jax.numpy as jnp
import math
from jax import lax

BATCH_ROWS = 96
SEQ_LEN = 1024
D_MODEL = 4096
N_HEADS = 16
HEAD_DIM = 256
GAIN_BLOCK = 32


def setup_inputs(seed: int = 0, part: int = 0) -> dict:
    root = jax.random.key(seed)
    shared = jax.random.split(root, 4)
    local = jax.random.split(jax.random.fold_in(root, part), 5)
    q_width = N_HEADS * HEAD_DIM
    align_scale = (math.log(SEQ_LEN) + 0.5) * HEAD_DIM ** -0.5
    tokens = jax.random.normal(local[0], (BATCH_ROWS, D_MODEL), jnp.float32)
    key_raw = jax.random.normal(shared[1], (D_MODEL, HEAD_DIM), jnp.float32)
    w_query = (jax.random.normal(shared[0], (D_MODEL, q_width), jnp.float32) + align_scale * jnp.tile(key_raw, (1, N_HEADS))) * D_MODEL ** -0.5
    w_key = key_raw * D_MODEL ** -0.5
    w_value = jax.random.normal(shared[2], (D_MODEL, HEAD_DIM), jnp.float32) * D_MODEL ** -0.5
    w_out = jax.random.normal(shared[3], (q_width, D_MODEL), jnp.float32) * q_width ** -0.5
    n_blocks = SEQ_LEN // GAIN_BLOCK
    key_gains = jax.random.uniform(local[1], (BATCH_ROWS, n_blocks, 1, 1), jnp.float32, 0.6, 1.6)
    k_cache = (jax.random.normal(local[2], (BATCH_ROWS, n_blocks, GAIN_BLOCK, HEAD_DIM), jnp.float32) * key_gains).reshape(BATCH_ROWS, SEQ_LEN, HEAD_DIM)
    v_cache = jax.random.normal(local[3], (BATCH_ROWS, SEQ_LEN, HEAD_DIM), jnp.float32)
    positions = jax.random.randint(local[4], (BATCH_ROWS,), SEQ_LEN // 4, SEQ_LEN, jnp.int32)
    positions = positions.at[0].set(SEQ_LEN - 1).at[1].set(SEQ_LEN // 4)
    return dict(tokens=tokens.astype(jnp.bfloat16), w_query=w_query.astype(jnp.bfloat16), w_key=w_key.astype(jnp.bfloat16), w_value=w_value.astype(jnp.bfloat16), w_out=w_out.astype(jnp.bfloat16), k_cache=k_cache.astype(jnp.bfloat16), v_cache=v_cache.astype(jnp.bfloat16), positions=positions)


def reference(tokens, w_query, w_key, w_value, w_out, k_cache, v_cache, positions):
    queries = jnp.dot(tokens, w_query, preferred_element_type=jnp.float32).astype(jnp.bfloat16)
    queries = queries.reshape(BATCH_ROWS, N_HEADS, HEAD_DIM)
    key_new = jnp.dot(tokens, w_key, preferred_element_type=jnp.float32).astype(jnp.bfloat16)
    value_new = jnp.dot(tokens, w_value, preferred_element_type=jnp.float32).astype(jnp.bfloat16)
    slot_ids = jnp.arange(SEQ_LEN)
    hit_mask = (slot_ids[None, :] == positions[:, None])[:, :, None]
    k_upd = jnp.where(hit_mask, key_new[:, None, :], k_cache)
    v_upd = jnp.where(hit_mask, value_new[:, None, :], v_cache)

    def one_row(row_args):
        q_row, k_row, v_row, pos_row = row_args
        scores = jnp.dot(q_row, k_row.T, preferred_element_type=jnp.float32) * HEAD_DIM ** -0.5
        scores = jnp.where(slot_ids[None, :] <= pos_row, scores, -jnp.inf)
        weights = jnp.exp(scores - jnp.max(scores, axis=1, keepdims=True))
        weight_sum = jnp.sum(weights, axis=1)
        value_sum = jnp.dot(weights.astype(jnp.bfloat16), v_row, preferred_element_type=jnp.float32)
        return value_sum / weight_sum[:, None]

    head_outs = lax.map(one_row, (queries, k_upd, v_upd, positions))
    attn_heads = head_outs.astype(jnp.bfloat16).reshape(BATCH_ROWS, N_HEADS * HEAD_DIM)
    attn_out = jnp.dot(attn_heads, w_out, preferred_element_type=jnp.float32).astype(jnp.bfloat16)
    return (attn_out, k_upd, v_upd)
```

```python
import functools

import jax
import jax.numpy as jnp
from jax import lax
from jax.experimental import pallas as pl
from jax.experimental.pallas import tpu as pltpu
from jax.sharding import PartitionSpec as P

F32, BF16 = jnp.float32, jnp.bfloat16
MESH = pl.DeviceIdType.MESH
LOWEST = float(jnp.finfo(jnp.float32).min)
STACK = 4
CHUNKS = 2
SPARE = 8


def attend_kernel(cfg, x_hbm, wq_hbm, wk_hbm, wv_hbm, wo_hbm, k_hbm, v_hbm, pos_ref, y_hbm, kn_hbm, vn_hbm,
                  xv, wq, wkv, wo, kc, vc, q_all, kv_new, kv_f32, q_f32, o_own, o_par, ml_own, ml_par,
                  o_send, o_recv, ml_send, ml_recv, y_own, y_out, y_par, y_send, y_recv, y_all,
                  in_sem, wq_sem, out_sem, yout_sem, q_sem, kv_sem, par_sem, ring_sem, mring_sem, ypar_sem, yring_sem, ag_sem, agp_sem):
    n_sp, n_rows, n_heads, hd, seq_local = cfg
    nz = n_sp // 2
    half = n_heads // 2
    hops = nz // 2
    rows = n_rows // CHUNKS
    pitch = n_rows + SPARE
    lt = hd // 128
    yblk = y_all.shape[2]
    per_tile = STACK * n_heads
    scale = hd ** -0.5
    me = lax.axis_index('sp')
    z, core = me // 2, me % 2
    other = 1 - core
    partner = {'sp': z * 2 + other}
    nbr = ({'sp': lax.rem(z + 1, nz) * 2 + core}, {'sp': lax.rem(z + nz - 1, nz) * 2 + core})

    def local(src, dst, sem):
        return pltpu.make_async_copy(src, dst, sem)

    x_in = local(x_hbm, xv, in_sem.at[0])
    x_in.start()

    def wq_in(i):
        col = pl.multiple_of((2 * i + core) * hd, hd)
        return local(wq_hbm.at[:, pl.ds(col, hd)], wq.at[i], wq_sem.at[i])

    for i in range(half):
        wq_in(i).start()

    @pl.when(core == 0)
    def _():
        local(wk_hbm, wkv, in_sem.at[1]).start()

    @pl.when(core == 1)
    def _():
        local(wv_hbm, wkv, in_sem.at[1]).start()

    k_in = local(k_hbm, kc, in_sem.at[2])
    v_in = local(v_hbm, vc, in_sem.at[3])
    k_in.start()
    v_in.start()
    d_model = y_hbm.shape[1]
    dh = d_model // 2
    wo_in = [local(wo_hbm.at[:, pl.ds(p * dh, dh)], wo.at[p], in_sem.at[4 + p]) for p in range(2)]
    for c in wo_in:
        c.start()

    barrier = pltpu.get_barrier_semaphore()
    for dev in (partner, *nbr):
        pl.semaphore_signal(barrier, inc=1, device_id=dev, device_id_type=MESH)
    pl.semaphore_wait(barrier, 3)

    def remote(src, dst, sems, dev):
        return pltpu.make_async_remote_copy(src_ref=src, dst_ref=dst, send_sem=sems.at[0], recv_sem=sems.at[1],
                                            device_id=dev, device_id_type=MESH)

    def q_copy(i, c):
        g = c * half + i
        return remote(q_all.at[g], q_all.at[g], q_sem.at[i], partner)

    def widen(g, q):
        r = pl.ds(pl.multiple_of(g * pitch, 8), n_rows)
        for i in range(lt):
            q_f32[i, r, :] = q[:, i * 128:(i + 1) * 128].astype(F32)

    x_in.wait()

    def q_head(i, carry):
        wq_in(i).wait()
        q = jnp.dot(xv[...], wq[i], preferred_element_type=F32).astype(BF16)
        g = core * half + i
        q_all[g] = q
        q_copy(i, core).start()
        widen(g, q)
        return carry

    lax.fori_loop(0, half, q_head, 0)
    local(wk_hbm, wkv, in_sem.at[1]).wait()
    kv_new[core] = jnp.dot(xv[...], wkv[...], preferred_element_type=F32).astype(BF16)
    kv_copy = remote(kv_new.at[core], kv_new.at[core], kv_sem, partner)
    kv_copy.start()

    def q_other(i, carry):
        q_copy(i, core).wait()
        g = other * half + i
        widen(g, q_all[g])
        return carry

    lax.fori_loop(0, half, q_other, 0)
    kv_copy.wait()
    kv_f32[...] = kv_new[...].astype(F32)
    kv_out = [local(kv_new.at[0], kn_hbm, out_sem.at[0]), local(kv_new.at[1], vn_hbm, out_sem.at[1])]
    for c in kv_out:
        c.start()
    k_in.wait()
    v_in.wait()

    width = STACK * seq_local
    row_seq = lax.broadcasted_iota(jnp.int32, (per_tile, 1), 0) // n_heads
    col = lax.broadcasted_iota(jnp.int32, (1, width), 1)
    col_seq, col_t = col // seq_local, col % seq_local
    lane = lax.broadcasted_iota(jnp.int32, (per_tile, 128), 1)
    base = me * seq_local

    def tile(j, carry):
        b0 = j * STACK
        slots = [pos_ref[b0 + s] - base for s in range(STACK)]
        slot_col, slot_row = jnp.full((1, width), slots[0]), jnp.full((per_tile, 1), slots[0])
        for s in range(1, STACK):
            slot_col = jnp.where(col_seq == s, slots[s], slot_col)
            slot_row = jnp.where(row_seq == s, slots[s], slot_row)
        keep = (row_seq == col_seq) & (col_t < slot_col)
        holds = (slot_row >= 0) & (slot_row < seq_local)
        q = jnp.concatenate([jnp.concatenate([q_f32[i, pl.ds(b0 + s, n_heads, stride=pitch), :] for i in range(lt)], axis=1)
                             for s in range(STACK)], axis=0)
        kn = jnp.concatenate([jnp.broadcast_to(kv_f32[0, pl.ds(b0 + s, 1), :], (n_heads, hd)) for s in range(STACK)], axis=0)
        vn = jnp.concatenate([jnp.broadcast_to(kv_f32[1, pl.ds(b0 + s, 1), :], (n_heads, hd)) for s in range(STACK)], axis=0)
        sc = lax.dot_general(q.astype(BF16), kc[j], (((1,), (1,)), ((), ())), preferred_element_type=F32) * scale
        sc = jnp.where(keep, sc, -jnp.inf)
        s_new = jnp.sum(q * kn, axis=1, keepdims=True) * scale
        s_new = jnp.where(holds, s_new, -jnp.inf)
        peak = jnp.maximum(jnp.maximum(jnp.max(sc, axis=1, keepdims=True), s_new), LOWEST)
        w = jnp.exp(sc - peak)
        w_new = jnp.exp(s_new - peak)
        total = jnp.sum(w, axis=1, keepdims=True) + w_new
        o = jnp.dot(w.astype(BF16), vc[j], preferred_element_type=F32) + w_new.astype(BF16).astype(F32) * vn
        ml = jnp.where(lane == 0, peak, total)
        for s in range(STACK):
            at = pl.ds(b0 + s, n_heads, stride=pitch)
            for i in range(lt):
                o_own[i, at, :] = o[s * n_heads:(s + 1) * n_heads, i * 128:(i + 1) * 128]
            ml_own[at, :] = ml[s * n_heads:(s + 1) * n_heads]
        return carry

    def part_rows(i, ch):
        return pl.ds(pl.multiple_of(i * pitch + ch * rows, 8), rows)

    def par_copies(i, ch):
        src, dst = part_rows(other * half + i, ch), part_rows(i, ch)
        return (remote(o_own.at[:, src], o_par.at[:, dst], par_sem.at[0, i, ch], partner),
                remote(ml_own.at[src], ml_par.at[dst], par_sem.at[1, i, ch], partner))

    tiles = n_rows // STACK // CHUNKS
    for ch in range(CHUNKS):
        lax.fori_loop(ch * tiles, (ch + 1) * tiles, tile, 0)
        for i in range(half):
            for c in par_copies(i, ch):
                c.start()

    for ch in range(CHUNKS):
        for i in range(half):
            for c in par_copies(i, ch):
                c.wait()

    lane_r = lax.broadcasted_iota(jnp.int32, (rows, 128), 1)
    row_r = lax.broadcasted_iota(jnp.int32, (rows, 128), 0)

    def to_row(m, l):
        return jnp.sum(jnp.where(lane_r == row_r, m, jnp.where(lane_r == row_r + 64, l, 0.0)), axis=0, keepdims=True)

    def to_cols(ml):
        m = jnp.sum(jnp.where(lane_r == row_r, ml, 0.0), axis=1, keepdims=True)
        l = jnp.sum(jnp.where(lane_r == row_r + 64, ml, 0.0), axis=1, keepdims=True)
        return m, l

    def own_terms(d, ch):
        a, b = part_rows(core * half + d, ch), part_rows(d, ch)
        return [([o_own[i, a, :] for i in range(lt)], ml_own[a, 0:1], ml_own[a, 1:2]),
                ([o_par[i, b, :] for i in range(lt)], ml_par[b, 0:1], ml_par[b, 1:2])]

    def merge(terms):
        top = functools.reduce(jnp.maximum, [m for _, m, _ in terms])
        f = [jnp.exp(m - top) for _, m, _ in terms]
        o = [sum(t[0][i] * f_t for t, f_t in zip(terms[1:], f[1:])) + terms[0][0][i] * f[0] for i in range(lt)]
        return o, top, sum(t[2] * f_t for t, f_t in zip(terms, f))

    def ring_copies(w, t, ch):
        return (remote(o_send.at[w, t, ch], o_recv.at[w, t, ch], ring_sem.at[w, t, ch], nbr[w]),
                remote(ml_send.at[w, t, ch], ml_recv.at[w, t, ch], mring_sem.at[w, t, ch], nbr[w]))

    def sends(w, t, ch):
        return t > 0 or ch % 2 == w

    def dest(w, t):
        dist = hops - t
        return lax.rem(z + (dist if w == 0 else nz - dist), nz)

    def received(w, t, ch):
        for c in ring_copies(w, t, ch):
            c.wait_recv()
        m, l = to_cols(ml_recv[w, t, ch])
        return ([o_recv[w, t, ch, i] for i in range(lt)], m, l)

    for t in range(hops):
        for ch in range(CHUNKS):
            for w in range(2):
                if not sends(w, t, ch):
                    continue
                terms = own_terms(dest(w, t), ch)
                if t > 0 and sends(w, t - 1, ch):
                    terms.append(received(w, t - 1, ch))
                o, m, l = merge(terms)
                for i in range(lt):
                    o_send[w, t, ch, i] = o[i]
                ml_send[w, t, ch] = to_row(m, l)
                for c in ring_copies(w, t, ch):
                    c.start()

    for c in wo_in:
        c.wait()

    def ypar_copy(i, ch):
        return remote(y_out.at[i, pl.ds(ch * rows, rows)], y_par.at[i, pl.ds(ch * rows, rows)], ypar_sem.at[i, ch], partner)

    for ch in range(CHUNKS):
        o, _, l = merge(own_terms(z, ch) + [received(w, hops - 1, ch) for w in range(2)])
        head = jnp.concatenate([o_i / l for o_i in o], axis=1).astype(BF16)
        there = jnp.dot(head, wo[other], preferred_element_type=F32)
        for i in range(nz):
            y_out[i, pl.ds(ch * rows, rows), :] = there[:, i * yblk:(i + 1) * yblk]
        for i in range(nz):
            ypar_copy(i, ch).start()
        here = jnp.dot(head, wo[core], preferred_element_type=F32)
        for i in range(nz):
            y_own[i, pl.ds(ch * rows, rows), :] = here[:, i * yblk:(i + 1) * yblk]

    def yring_copy(w, t, ch):
        return remote(y_send.at[w, t, ch], y_recv.at[w, t, ch], yring_sem.at[w, t, ch], nbr[w])

    for ch in range(CHUNKS):
        for i in range(nz):
            ypar_copy(i, ch).wait()

    def y_terms(d, ch):
        r = pl.ds(ch * rows, rows)
        return y_own[d, r, :] + y_par[d, r, :]

    for t in range(hops):
        for ch in range(CHUNKS):
            for w in range(2):
                if not sends(w, t, ch):
                    continue
                part = y_terms(dest(w, t), ch)
                if t > 0 and sends(w, t - 1, ch):
                    yring_copy(w, t - 1, ch).wait_recv()
                    part = part + y_recv[w, t - 1, ch]
                y_send[w, t, ch] = part
                yring_copy(w, t, ch).start()

    def ag_copy(w, t, ch):
        src = lax.rem(z + (nz - t if w == 0 else t), nz)
        ref = y_all.at[core * half + src, pl.ds(ch * rows, rows)]
        return remote(ref, ref, ag_sem.at[w, t, ch], nbr[w])

    def ag_recv(w, t, ch):
        src = lax.rem(z + (nz - t - 1 if w == 0 else t + 1), nz)
        ref = y_all.at[core * half + src, pl.ds(ch * rows, rows)]
        return remote(ref, ref, ag_sem.at[w, t, ch], nbr[w])

    def agp_copy(src, ch, c):
        ref = y_all.at[c * half + src, pl.ds(ch * rows, rows)]
        return remote(ref, ref, agp_sem.at[src, ch], partner)

    def y_block_out(c, src, ch):
        r = pl.ds(ch * rows, rows)
        at = pl.multiple_of((c * half + src) * yblk, yblk)
        return local(y_all.at[c * half + src, r], y_hbm.at[r, pl.ds(at, yblk)], yout_sem.at[c, src, ch])

    def gathers(w, t, ch):
        return t < hops - 1 or ch % 2 == w

    for ch in range(CHUNKS):
        part = y_terms(z, ch)
        for w in range(2):
            yring_copy(w, hops - 1, ch).wait_recv()
            part = part + y_recv[w, hops - 1, ch]
        y_all[core * half + z, pl.ds(ch * rows, rows), :] = part.astype(BF16)
        for w in range(2):
            if gathers(w, 0, ch):
                ag_copy(w, 0, ch).start()
        agp_copy(z, ch, core).start()
        y_block_out(core, z, ch).start()

    for t in range(hops):
        for ch in range(CHUNKS):
            for w in range(2):
                if not gathers(w, t, ch):
                    continue
                ag_recv(w, t, ch).wait_recv()
                if t + 1 < hops and gathers(w, t + 1, ch):
                    ag_copy(w, t + 1, ch).start()
                src = lax.rem(z + (nz - t - 1 if w == 0 else t + 1), nz)
                agp_copy(src, ch, core).start()
                y_block_out(core, src, ch).start()

    def order():
        yield z
        for t in range(hops):
            yield lax.rem(z + nz - t - 1, nz)
            if t < hops - 1:
                yield lax.rem(z + t + 1, nz)

    for src in order():
        for ch in range(CHUNKS):
            agp_copy(src, ch, other).wait_recv()
            y_block_out(other, src, ch).start()

    for src in range(nz):
        for ch in range(CHUNKS):
            agp_copy(src, ch, core).wait_send()
            for c in range(2):
                y_block_out(c, src, ch).wait()
    for t in range(hops):
        for ch in range(CHUNKS):
            for w in range(2):
                if sends(w, t, ch):
                    for c in ring_copies(w, t, ch):
                        c.wait_send()
                    yring_copy(w, t, ch).wait_send()
                if gathers(w, t, ch):
                    ag_copy(w, t, ch).wait_send()
    for c in kv_out:
        c.wait()


def attend(cfg, *args):
    n_sp, n_rows, n_heads, hd, seq_local = cfg
    x, w_query, w_key, w_value, w_out, k, v, pos = args
    nz, half, hops, rows = n_sp // 2, n_heads // 2, n_sp // 4, n_rows // CHUNKS
    d_model, yblk, stacks = x.shape[1], w_out.shape[1] // n_sp, n_rows // STACK
    width, pitch, lt = STACK * seq_local, n_rows + SPARE, hd // 128
    dma = lambda *s: pltpu.SemaphoreType.DMA(s)
    any_spec = pl.BlockSpec(memory_space=pl.ANY)
    return pl.pallas_call(
        functools.partial(attend_kernel, cfg),
        name='attend',
        out_shape=(jax.ShapeDtypeStruct((n_rows, w_out.shape[1]), BF16),
                   jax.ShapeDtypeStruct((n_rows, hd), BF16),
                   jax.ShapeDtypeStruct((n_rows, hd), BF16)),
        in_specs=[any_spec] * 7 + [pl.BlockSpec(memory_space=pltpu.SMEM)],
        out_specs=(any_spec,) * 3,
        scratch_shapes=[
            pltpu.VMEM((n_rows, d_model), BF16),
            pltpu.VMEM((half, d_model, hd), BF16),
            pltpu.VMEM((d_model, hd), BF16),
            pltpu.VMEM((2, hd, w_out.shape[1] // 2), BF16),
            pltpu.VMEM((stacks, width, hd), BF16),
            pltpu.VMEM((stacks, width, hd), BF16),
            pltpu.VMEM((n_heads, n_rows, hd), BF16),
            pltpu.VMEM((2, n_rows, hd), BF16),
            pltpu.VMEM((2, n_rows, hd), F32),
            pltpu.VMEM((lt, n_heads * pitch, 128), F32),
            pltpu.VMEM((lt, n_heads * pitch, 128), F32),
            pltpu.VMEM((lt, half * pitch, 128), F32),
            pltpu.VMEM((n_heads * pitch, 128), F32),
            pltpu.VMEM((half * pitch, 128), F32),
            pltpu.VMEM((2, hops, CHUNKS, lt, rows, 128), F32),
            pltpu.VMEM((2, hops, CHUNKS, lt, rows, 128), F32),
            pltpu.VMEM((2, hops, CHUNKS, 1, 128), F32),
            pltpu.VMEM((2, hops, CHUNKS, 1, 128), F32),
            pltpu.VMEM((nz, n_rows, yblk), F32),
            pltpu.VMEM((nz, n_rows, yblk), F32),
            pltpu.VMEM((nz, n_rows, yblk), F32),
            pltpu.VMEM((2, hops, CHUNKS, rows, yblk), F32),
            pltpu.VMEM((2, hops, CHUNKS, rows, yblk), F32),
            pltpu.VMEM((n_sp, n_rows, yblk), BF16),
            dma(6), dma(half), dma(2), dma(2, nz, CHUNKS),
            dma(half, 2), dma(2), dma(2, half, CHUNKS, 2),
            dma(2, hops, CHUNKS, 2), dma(2, hops, CHUNKS, 2), dma(nz, CHUNKS, 2),
            dma(2, hops, CHUNKS, 2), dma(2, hops, CHUNKS, 2), dma(nz, CHUNKS, 2),
        ],
        compiler_params=pltpu.CompilerParams(collective_id=0, has_side_effects=True, vmem_limit_bytes=60 * 1024 * 1024),
        cost_estimate=pl.CostEstimate(flops=10**9, bytes_accessed=3 * 10**7, transcendentals=0),
    )(x, w_query, w_key, w_value, w_out, k.reshape(stacks, width, hd), v.reshape(stacks, width, hd), pos)


def solution(mesh):
    n_sp = mesh.shape['sp']

    def local_step(tokens, w_query, w_key, w_value, w_out, k_cache, v_cache, positions):
        n_rows, seq_local, hd = k_cache.shape
        cfg = (n_sp, n_rows, w_query.shape[1] // hd, hd, seq_local)
        attn_out, key_new, value_new = attend(cfg, tokens, w_query, w_key, w_value, w_out, k_cache, v_cache, positions)
        local_pos = positions - lax.axis_index('sp') * seq_local
        hit = (jnp.arange(seq_local)[None, :] == local_pos[:, None])[:, :, None]
        return attn_out, jnp.where(hit, key_new[:, None, :], k_cache), jnp.where(hit, value_new[:, None, :], v_cache)

    cache_spec = P('dp', 'sp', None)
    return jax.shard_map(local_step, mesh=mesh,
                         in_specs=(P('dp', None), P(), P(), P(), P('sp', None), cache_spec, cache_spec, P('dp')),
                         out_specs=(P('dp', None), cache_spec, cache_spec), check_vma=False)
```
